32 devices in a mesh: zero: 16 (over z, x, core), tensor: 2 (over y).
Axes of the slice: x: 2, y: 2, z: 4, core: 2. Of those that a mesh axis runs over, the one named last changes fastest.
Arguments:
- grads: bfloat16 [16, 2, 16, 49152], P('zero', None, None, 'tensor'), may hold values from -1200 to 1200
- moment1: bfloat16 [2, 16, 49152], P(None, 'zero', 'tensor'), may hold values from -1 to 1
- moment2: float32 [2, 16, 49152], P(None, 'zero', 'tensor'), may hold values from 0.01 to 0.2
- master: float32 [2, 16, 49152], P(None, 'zero', 'tensor'), may hold values from -0.008 to 0.008
Outputs:
- new_moment1: bfloat16 [2, 16, 49152], P(None, 'zero', 'tensor')
- new_moment2: float32 [2, 16, 49152], P(None, 'zero', 'tensor')
- new_master: float32 [2, 16, 49152], P(None, 'zero', 'tensor')
- weights: bfloat16 [2, 16, 49152], P(None, None, 'tensor')
The draws below stay inside these ranges and needn't reach their ends.
All inputs are finite; a program needn't handle non-finite values. Where the reference program divides by a largest or mean magnitude, that divisor is 1e-20 or more.
Results may differ from the reference program's by a relative error of at most 0.0053.
Values may be sent and summed in bfloat16 or wider, within the bound.
A program may use at most 64 MiB of HBM per device.

```python
import math
import jax
import jax.numpy as jnp
from jax import lax

FF = 49152
LAYERS = 2
ROW_DEV = 1
ROWS = 16
N_TENSOR = 2


def draw_grads(key, part):
    keys = jax.random.split(key, 3)
    replicas = ROWS // ROW_DEV
    shape = (replicas, LAYERS, ROWS, FF)
    base = jnp.clip(jax.random.normal(keys[0], shape, jnp.float32), -4.0, 4.0)
    row_scale = jnp.exp(jax.random.uniform(keys[1], (LAYERS, ROWS), jnp.float32, 0.0, math.log(10.0)))
    col_scale = jnp.exp(jax.random.uniform(keys[2], (FF,), jnp.float32, 0.0, math.log(3.0)))
    rising = 1.0 + 2.0 * jnp.arange(replicas, dtype=jnp.float32) / max(replicas - 1, 1)
    shard_rise = 1.0 + 2.0 * (jnp.arange(FF) // (FF // N_TENSOR)).astype(jnp.float32) / max(N_TENSOR - 1, 1)
    values = base * row_scale[None, :, :, None] * (col_scale * shard_rise)[None, None, None, :]
    values = values * rising[:, None, None, None]
    return values.astype(jnp.bfloat16)


def draw_master(key, part):
    keys = jax.random.split(key, 3)
    shape = (LAYERS, ROWS, FF)
    base = jnp.clip(jax.random.normal(keys[0], shape, jnp.float32), -4.0, 4.0)
    row_scale = jnp.exp(jax.random.uniform(keys[1], (LAYERS, ROWS), jnp.float32, 0.0, math.log(10.0)))
    col_scale = jnp.exp(jax.random.uniform(keys[2], (FF,), jnp.float32, 0.0, math.log(3.0)))
    rising = 1.0 + 2.0 * jnp.arange(ROWS, dtype=jnp.float32) / max(ROWS - 1, 1)
    values = 2e-05 * base * (row_scale * rising[None, :])[:, :, None] * col_scale[None, None, :]
    return values.astype(jnp.float32)


def block_levels(stream_key, shape, pieces, smallest, largest):
    factor_of = 1.0
    for axis_at, blocks in pieces:
        heights = jax.random.uniform(jax.random.fold_in(jax.random.fold_in(stream_key, 6), axis_at), (blocks,), jnp.float32, smallest / len(pieces), largest / len(pieces))
        factor_of = factor_of * jnp.repeat(jnp.exp(heights), shape[axis_at] // blocks).reshape((-1,) + (1,) * (len(shape) - 1 - axis_at))
    return factor_of


def normal_values(own_key, shape, deviation, most, cuts=(), held_as=jnp.bfloat16):
    values = jax.random.normal(own_key, shape, jnp.float32) * deviation
    if len(cuts) > 0:
        values = block_levels(own_key, shape, cuts, -0.22, 0.18) * values
    return jnp.clip(values, min=-most, max=most).astype(held_as)


def setup_inputs(seed: int = 0) -> dict:
    streams_of = jax.random.split(jax.random.key(seed), 5)
    grads = draw_grads(jax.random.fold_in(streams_of[4], 71), 0)
    moment1 = normal_values(streams_of[1], (LAYERS, ROWS, FF), 0.2, 1.0, ((1, 16), (2, 2)))
    moment2 = jnp.clip(jnp.exp(math.log(0.2) - 2.9957323 * jax.random.uniform(streams_of[2], (LAYERS, ROWS, FF), jnp.float32) ** block_levels(streams_of[2], (LAYERS, ROWS, FF), ((1, 16), (2, 2)), -0.2, 0.2)), 0.01, 0.2)
    master = draw_master(jax.random.fold_in(streams_of[4], 71), 0)
    return dict(grads=grads, moment1=moment1, moment2=moment2, master=master)


decay_first = 0.9
decay_second = 0.95
learn_rate = 0.001
weight_decay = 0.1
adam_epsilon = 1e-08
peak_epsilon = 1e-06
bias_first = 1.0 - 0.9 ** 10
bias_second = 1.0 - 0.95 ** 10

def reference(grads, moment1, moment2, master):
    peak = lax.optimization_barrier(jnp.max(jnp.abs(grads), axis=(0, 2, 3))).astype(jnp.float32) + peak_epsilon

    def add_replica(total, replica):
        scaled = (replica.astype(jnp.float32) / peak[:, None, None]).astype(jnp.bfloat16)
        scaled = lax.optimization_barrier(scaled)
        return (total + scaled.astype(jnp.float32), None)
    start = jnp.zeros(moment2.shape, jnp.float32)
    gsum, unused = lax.scan(add_replica, start, grads)
    new_moment1 = (decay_first * moment1.astype(jnp.float32) + (1.0 - decay_first) * gsum).astype(jnp.bfloat16)
    new_moment2 = decay_second * moment2 + (1.0 - decay_second) * gsum * gsum
    stored = lax.optimization_barrier(new_moment1).astype(jnp.float32)
    step_dir = stored / bias_first / (jnp.sqrt(new_moment2 / bias_second) + adam_epsilon)
    new_master = master - learn_rate * (step_dir + weight_decay * master)
    wpeak = lax.optimization_barrier(jnp.max(jnp.abs(new_master), axis=(1, 2))) + peak_epsilon
    weights = (new_master / wpeak[:, None, None]).astype(jnp.bfloat16)
    return (new_moment1, new_moment2, new_master, weights)
```

```python
import functools

import jax
import jax.numpy as jnp
from jax import lax
from jax.experimental import pallas as pl
from jax.experimental.pallas import tpu as pltpu
from jax.sharding import PartitionSpec as P

decay_first = 0.9
decay_second = 0.95
learn_rate = 0.001
weight_decay = 0.1
adam_epsilon = 1e-08
peak_epsilon = 1e-06
bias_first = 1.0 - 0.9**10
bias_second = 1.0 - 0.95**10

LANES = 128
MESH = pl.DeviceIdType.MESH
f32 = jnp.float32
bf16 = jnp.bfloat16


def split_zero(n):
    nc = 2 if n % 2 == 0 else 1
    m = n // nc
    nx = 1
    while (nx * 2) * (nx * 2) <= m and m % (nx * 2) == 0:
        nx *= 2
    return m // nx, nx, nc


def fold(block):
    return jnp.max(jnp.abs(block.astype(f32)).reshape(-1, 8, LANES), axis=0)


def kernel(dims, g_ref, m1_ref, m2_ref, ms_ref,
           o1_ref, o2_ref, om_ref, wg_ref, wp_ref,
           buf_c, send_x, buf_x, send_z, buf_z, own,
           pk, pk_in, wk, wk_in,
           cs, cr, xs, xr, zs, zr, gzs, gzr, gxs, gxr, gcs, gcr, ps, pr, ws, wr):
    nz, nx, nc, nt, nl = dims
    me = lax.axis_index("zero")
    te = lax.axis_index("tensor")
    c = lax.rem(me, nc)
    x = lax.rem(lax.div(me, nc), nx)
    z = lax.div(me, nc * nx)

    def at(zz, xx, cc):
        return {"zero": (zz * nx + xx) * nc + cc}

    def turn(v, d, n):
        return lax.rem(v + d, n)

    core_peers = [at(z, x, turn(c, d, nc)) for d in range(1, nc)]
    x_peers = [at(z, turn(x, d, nx), c) for d in range(1, nx)]
    z_peers = [at(turn(z, d, nz), x, c) for d in range(1, nz)]
    t_peers = [{"tensor": turn(te, d, nt)} for d in range(1, nt)]
    groups = [p for p in (core_peers, x_peers, z_peers, t_peers) if p]
    pending = []

    def send(src, dst, s, r, to):
        copy = pltpu.make_async_remote_copy(
            src_ref=src, dst_ref=dst, send_sem=s, recv_sem=r,
            device_id=to, device_id_type=MESH)
        copy.start()
        pending.append(copy)

    def arrived(dst, r):
        pltpu.make_async_copy(dst, dst, r).wait()

    barrier = pltpu.get_barrier_semaphore()
    everyone = [p for g in groups for p in g]
    for p in everyone:
        pl.semaphore_signal(barrier, inc=1, device_id=p, device_id_type=MESH)

    class Peak:
        def __init__(self, held, inbox, s, r):
            self.held, self.inbox, self.s, self.r = held, inbox, s, r
            self.stage = 0
            self.slot = 0

        def push(self):
            for i, p in enumerate(groups[self.stage]):
                k = self.slot + i
                send(self.held.at[self.stage], self.inbox.at[k], self.s.at[k], self.r.at[k], p)

        def pull(self):
            best = self.held[self.stage]
            for i in range(len(groups[self.stage])):
                k = self.slot + i
                arrived(self.inbox.at[k], self.r.at[k])
                best = jnp.maximum(best, self.inbox[k])
            self.slot += len(groups[self.stage])
            self.stage += 1
            self.held[self.stage] = best
            if self.stage < len(groups):
                self.push()

        def step(self):
            if self.stage < len(groups):
                self.pull()

        def finish(self):
            while self.stage < len(groups):
                self.pull()
            return [jnp.max(self.held[self.stage, l]) + peak_epsilon for l in range(nl)]

    for l in range(nl):
        def part(i, best, l=l):
            zz, rest = lax.div(i, nx * nc), lax.rem(i, nx * nc)
            return jnp.maximum(best, fold(g_ref[zz, lax.div(rest, nc), lax.rem(rest, nc), l]))
        pk[0, l] = lax.fori_loop(0, nz * nx * nc, part, jnp.zeros((8, LANES), f32))

    pl.semaphore_wait(barrier, len(everyone))

    order = [(d, l) for d in list(range(1, nz)) + [0] for l in range(nl)]
    other = [turn(c, d, nc) for d in range(1, nc)]
    for d, l in order:
        zz = turn(z, d, nz)
        for i, cc in enumerate(other):
            send(g_ref.at[zz, :, cc, l], buf_c.at[i, d, l], cs.at[i, d, l], cr.at[i, d, l], core_peers[i])
    peak = Peak(pk, pk_in, ps, pr)
    peak.push()

    def pair(d, l, xx):
        total = g_ref[turn(z, d, nz), xx, c, l].astype(f32)
        for i in range(nc - 1):
            total = total + buf_c[i, d, l, xx].astype(f32)
        return total

    for k, (d, l) in enumerate(order):
        for i in range(nc - 1):
            arrived(buf_c.at[i, d, l], cr.at[i, d, l])
        for e in range(1, nx):
            send_x[e - 1, d, l] = pair(d, l, turn(x, e, nx)).astype(bf16)
            send(send_x.at[e - 1, d, l], buf_x.at[e - 1, d, l],
                 xs.at[e - 1, d, l], xr.at[e - 1, d, l], x_peers[e - 1])
    peak.step()
    for k, (d, l) in enumerate(order):
        for e in range(1, nx):
            arrived(buf_x.at[e - 1, d, l], xr.at[e - 1, d, l])
        total = pair(d, l, x)
        for e in range(1, nx):
            total = total + buf_x[e - 1, d, l].astype(f32)
        if d:
            send_z[d - 1, l] = total.astype(bf16)
            send(send_z.at[d - 1, l], buf_z.at[d - 1, l], zs.at[d - 1, l], zr.at[d - 1, l], z_peers[d - 1])
        else:
            own[l] = total
        if l == nl - 1:
            peak.step()
    peaks = peak.finish()

    for l in range(nl):
        total = own[l]
        for d in range(1, nz):
            arrived(buf_z.at[d - 1, l], zr.at[d - 1, l])
            total = total + buf_z[d - 1, l].astype(f32)
        gsum = total / peaks[l]
        first = (decay_first * m1_ref[l].astype(f32) + (1.0 - decay_first) * gsum).astype(bf16)
        second = decay_second * m2_ref[l] + (1.0 - decay_second) * gsum * gsum
        o1_ref[l] = first
        o2_ref[l] = second
        step_dir = first.astype(f32) / bias_first / (jnp.sqrt(second / bias_second) + adam_epsilon)
        master = ms_ref[l]
        fresh = master - learn_rate * (step_dir + weight_decay * master)
        om_ref[l] = fresh
        wg_ref[z, x, c, l] = fresh.astype(bf16)
        wk[0, l] = fold(fresh)
        mine = wg_ref.at[z, x, c, l]
        for d in range(1, nz):
            send(mine, mine, gzs.at[d - 1, l], gzr.at[d - 1, l], z_peers[d - 1])
        for e in range(1, nx):
            send(mine, mine, gxs.at[e - 1, 0, l], gxr.at[e - 1, 0, l], x_peers[e - 1])
        for i in range(1, nc):
            send(mine, mine, gcs.at[i - 1, 0, 0, l], gcr.at[i - 1, 0, 0, l], core_peers[i - 1])
    wpeak = Peak(wk, wk_in, ws, wr)
    wpeak.push()

    def back(v, d, n):
        return lax.rem(v + n - d, n)

    def from_z(d, l):
        block = wg_ref.at[back(z, d, nz), x, c, l]
        arrived(block, gzr.at[d - 1, l])
        for e in range(1, nx):
            send(block, block, gxs.at[e - 1, d, l], gxr.at[e - 1, d, l], x_peers[e - 1])
        for i in range(1, nc):
            send(block, block, gcs.at[i - 1, 0, d, l], gcr.at[i - 1, 0, d, l], core_peers[i - 1])

    def from_x(d, l):
        for e in range(1, nx):
            block = wg_ref.at[back(z, d, nz), back(x, e, nx), c, l]
            arrived(block, gxr.at[e - 1, d, l])
            for i in range(1, nc):
                send(block, block, gcs.at[i - 1, e, d, l], gcr.at[i - 1, e, d, l], core_peers[i - 1])

    wpeak.step()
    for d in range(1, nz):
        for l in range(nl):
            from_z(d, l)
        if d == 1:
            wpeak.step()
        for l in range(nl):
            from_x(d - 1, l)
    wpeak.step()
    for l in range(nl):
        from_x(nz - 1, l)
    peaks = wpeak.finish()
    for l in range(nl):
        wp_ref[l] = jnp.full((8, LANES), peaks[l], f32)
    for d in range(nz):
        for e in range(nx):
            for l in range(nl):
                for i in range(1, nc):
                    block = wg_ref.at[back(z, d, nz), back(x, e, nx), back(c, i, nc), l]
                    arrived(block, gcr.at[i - 1, e, d, l])
    for copy in pending:
        copy.wait_send()


def local(n, nt, grads, moment1, moment2, master):
    nz, nx, nc = split_zero(n)
    nl, rows, width = grads.shape[1:]
    deep = (rows // n) * width // LANES
    dims = (nz, nx, nc, nt, nl)
    g = grads.reshape(nl, n, deep, LANES).transpose(1, 0, 2, 3).reshape(nz, nx, nc, nl, deep, LANES)
    flat = (nl, deep, LANES)
    peers = (nc - 1) + (nx - 1) + (nz - 1) + (nt - 1)
    stages = sum(k > 1 for k in (nc, nx, nz, nt))
    c1, x1, z1 = max(nc - 1, 1), max(nx - 1, 1), max(nz - 1, 1)
    dma = pltpu.SemaphoreType.DMA
    tile = (nl, 8, LANES)
    vm = pl.BlockSpec(memory_space=pltpu.VMEM)
    sems = [dma((c1, nz, nl))] * 2 + [dma((x1, nz, nl))] * 2 + [dma((z1, nl))] * 2
    sems += [dma((z1, nl))] * 2 + [dma((x1, nz, nl))] * 2 + [dma((c1, nx, nz, nl))] * 2
    sems += [dma((peers,))] * 4
    o1, o2, om, wg, wp = pl.pallas_call(
        functools.partial(kernel, dims),
        out_shape=(
            jax.ShapeDtypeStruct(flat, bf16),
            jax.ShapeDtypeStruct(flat, f32),
            jax.ShapeDtypeStruct(flat, f32),
            jax.ShapeDtypeStruct((nz, nx, nc) + flat, bf16),
            jax.ShapeDtypeStruct(tile, f32),
        ),
        in_specs=[vm] * 4,
        out_specs=(vm,) * 5,
        scratch_shapes=[
            pltpu.VMEM((c1, nz, nl, nx, deep, LANES), bf16),
            pltpu.VMEM((x1, nz) + flat, bf16),
            pltpu.VMEM((x1, nz) + flat, bf16),
            pltpu.VMEM((z1,) + flat, bf16),
            pltpu.VMEM((z1,) + flat, bf16),
            pltpu.VMEM(flat, f32),
            pltpu.VMEM((stages + 1,) + tile, f32),
            pltpu.VMEM((peers,) + tile, f32),
            pltpu.VMEM((stages + 1,) + tile, f32),
            pltpu.VMEM((peers,) + tile, f32),
        ] + sems,
        compiler_params=pltpu.CompilerParams(collective_id=0, has_side_effects=True),
    )(g, moment1.reshape(flat), moment2.reshape(flat), master.reshape(flat))
    wg = wg.reshape((n,) + flat).astype(f32) / wp[:, :1, :1][None]
    weights = wg.astype(bf16).transpose(1, 0, 2, 3).reshape(nl, rows, width)
    shape = moment1.shape
    return o1.reshape(shape), o2.reshape(shape), om.reshape(shape), weights


def solution(mesh):
    n, nt = mesh.shape["zero"], mesh.shape["tensor"]
    placed = (
        P("zero", None, None, "tensor"),
        P(None, "zero", "tensor"),
        P(None, "zero", "tensor"),
        P(None, "zero", "tensor"),
    )
    return jax.shard_map(
        functools.partial(local, n, nt),
        mesh=mesh,
        in_specs=placed,
        out_specs=(
            P(None, "zero", "tensor"),
            P(None, "zero", "tensor"),
            P(None, "zero", "tensor"),
            P(None, None, "tensor"),
        ),
        check_vma=False,
    )
```

```python
import functools

import jax
import jax.numpy as jnp
from jax import lax
from jax.experimental import pallas as pl
from jax.experimental.pallas import tpu as pltpu
from jax.sharding import PartitionSpec as P

decay_first = 0.9
decay_second = 0.95
learn_rate = 0.001
weight_decay = 0.1
adam_epsilon = 1e-08
peak_epsilon = 1e-06
bias_first = 1.0 - 0.9**10
bias_second = 1.0 - 0.95**10

LANES = 128
MESH = pl.DeviceIdType.MESH
f32 = jnp.float32
bf16 = jnp.bfloat16


def split_zero(n):
    nc = 2 if n % 2 == 0 else 1
    m = n // nc
    nx = 1
    while (nx * 2) * (nx * 2) <= m and m % (nx * 2) == 0:
        nx *= 2
    return m // nx, nx, nc


def fold(block):
    return jnp.max(jnp.abs(block.astype(f32)).reshape(-1, 8, LANES), axis=0)


def kernel(dims, g_ref, m1_ref, m2_ref, ms_ref,
           o1_ref, o2_ref, om_ref, ow_ref,
           wg, m1_wide, o1_wide, buf_c, send_x, buf_x, send_z, buf_z, own,
           pk, pk_in, wk, wk_in,
           cs, cr, xs, xr, zs, zr, gzs, gzr, gxs, gxr, gcs, gcr, ps, pr, ws, wr):
    nz, nx, nc, nt, nl = dims
    me = lax.axis_index("zero")
    te = lax.axis_index("tensor")
    c = lax.rem(me, nc)
    x = lax.rem(lax.div(me, nc), nx)
    z = lax.div(me, nc * nx)

    def at(zz, xx, cc):
        return {"zero": (zz * nx + xx) * nc + cc}

    def turn(v, d, n):
        return lax.rem(v + d, n)

    core_peers = [at(z, x, turn(c, d, nc)) for d in range(1, nc)]
    x_peers = [at(z, turn(x, d, nx), c) for d in range(1, nx)]
    z_peers = [at(turn(z, d, nz), x, c) for d in range(1, nz)]
    t_peers = [{"tensor": turn(te, d, nt)} for d in range(1, nt)]
    near = core_peers + t_peers + [
        {**at(z, x, turn(c, i, nc)), "tensor": turn(te, d, nt)} for i in range(1, nc) for d in range(1, nt)]
    far = [at(turn(z, d, nz), turn(x, e, nx), c) for d in range(nz) for e in range(nx) if d or e]
    pending = []

    def send(src, dst, s, r, to):
        copy = pltpu.make_async_remote_copy(
            src_ref=src, dst_ref=dst, send_sem=s, recv_sem=r,
            device_id=to, device_id_type=MESH)
        copy.start()
        pending.append(copy)

    def arrived(dst, r):
        pltpu.make_async_copy(dst, dst, r).wait()

    barrier = pltpu.get_barrier_semaphore()
    everyone = near + far
    for p in everyone:
        pl.semaphore_signal(barrier, inc=1, device_id=p, device_id_type=MESH)

    class Peak:
        def __init__(self, held, inbox, s, r):
            self.held, self.inbox, self.s, self.r = held, inbox, s, r

        def push(self, stage):
            first = 0 if stage == 0 else len(near)
            for i, p in enumerate(near if stage == 0 else far):
                k = first + i
                send(self.held.at[stage], self.inbox.at[k], self.s.at[k], self.r.at[k], p)

        def pull(self, stage):
            first = 0 if stage == 0 else len(near)
            best = self.held[stage]
            for k in range(first, first + len(near if stage == 0 else far)):
                arrived(self.inbox.at[k], self.r.at[k])
                best = jnp.maximum(best, self.inbox[k])
            return best

        def relay(self):
            self.held[1] = self.pull(0)
            self.push(1)

        def finish(self):
            best = self.pull(1)
            return [jnp.max(best[l]) + peak_epsilon for l in range(nl)]

    for l in range(nl):
        def part(i, best, l=l):
            zz, rest = lax.div(i, nx * nc), lax.rem(i, nx * nc)
            return jnp.maximum(best, fold(g_ref[l, zz, lax.div(rest, nc), lax.rem(rest, nc)]))
        pk[0, l] = lax.fori_loop(0, nz * nx * nc, part, jnp.zeros((8, LANES), f32))

    pl.semaphore_wait(barrier, len(everyone))

    peak = Peak(pk, pk_in, ps, pr)
    peak.push(0)
    order = [(d, l) for d in list(range(1, nz)) + [0] for l in range(nl)]
    other = [turn(c, d, nc) for d in range(1, nc)]
    for d, l in order:
        zz = turn(z, d, nz)
        for i, cc in enumerate(other):
            send(g_ref.at[l, zz, :, cc], buf_c.at[i, d, l], cs.at[i, d, l], cr.at[i, d, l], core_peers[i])
    m1_wide[...] = m1_ref[...].astype(f32)

    def pair(d, l, xx):
        total = g_ref[l, turn(z, d, nz), xx, c].astype(f32)
        for i in range(nc - 1):
            total = total + buf_c[i, d, l, xx].astype(f32)
        return total

    for k, (d, l) in enumerate(order):
        for i in range(nc - 1):
            arrived(buf_c.at[i, d, l], cr.at[i, d, l])
        for e in range(1, nx):
            send_x[e - 1, d, l] = pair(d, l, turn(x, e, nx)).astype(bf16)
            send(send_x.at[e - 1, d, l], buf_x.at[e - 1, d, l],
                 xs.at[e - 1, d, l], xr.at[e - 1, d, l], x_peers[e - 1])
        if k == 0:
            peak.relay()
    for k, (d, l) in enumerate(order):
        for e in range(1, nx):
            arrived(buf_x.at[e - 1, d, l], xr.at[e - 1, d, l])
        total = pair(d, l, x)
        for e in range(1, nx):
            total = total + buf_x[e - 1, d, l].astype(f32)
        if d:
            send_z[d - 1, l] = total.astype(bf16)
            send(send_z.at[d - 1, l], buf_z.at[d - 1, l], zs.at[d - 1, l], zr.at[d - 1, l], z_peers[d - 1])
        else:
            own[l] = total
    peaks = peak.finish()

    for l in range(nl):
        total = own[l]
        for d in range(1, nz):
            arrived(buf_z.at[d - 1, l], zr.at[d - 1, l])
            total = total + buf_z[d - 1, l].astype(f32)
        gsum = total / peaks[l]
        first = (decay_first * m1_wide[:, l, :] + (1.0 - decay_first) * gsum).astype(bf16)
        second = decay_second * m2_ref[l] + (1.0 - decay_second) * gsum * gsum
        o1_wide[:, l, :] = first.astype(f32)
        o2_ref[l] = second
        step_dir = first.astype(f32) / bias_first / (jnp.sqrt(second / bias_second) + adam_epsilon)
        master = ms_ref[l]
        fresh = master - learn_rate * (step_dir + weight_decay * master)
        om_ref[l] = fresh
        wg[l, z, x, c] = fresh.astype(bf16)
        wk[0, l] = fold(fresh)
        mine = wg.at[l, z, x, c]
        for d in range(1, nz):
            send(mine, mine, gzs.at[d - 1, l], gzr.at[d - 1, l], z_peers[d - 1])
        for e in range(1, nx):
            send(mine, mine, gxs.at[e - 1, 0, l], gxr.at[e - 1, 0, l], x_peers[e - 1])
        for i in range(1, nc):
            send(mine, mine, gcs.at[i - 1, 0, 0, l], gcr.at[i - 1, 0, 0, l], core_peers[i - 1])
    wpeak = Peak(wk, wk_in, ws, wr)
    wpeak.push(0)
    o1_ref[...] = o1_wide[...].astype(bf16)

    def back(v, d, n):
        return lax.rem(v + n - d, n)

    def from_z(d, l):
        block = wg.at[l, back(z, d, nz), x, c]
        arrived(block, gzr.at[d - 1, l])
        for e in range(1, nx):
            send(block, block, gxs.at[e - 1, d, l], gxr.at[e - 1, d, l], x_peers[e - 1])
        for i in range(1, nc):
            send(block, block, gcs.at[i - 1, 0, d, l], gcr.at[i - 1, 0, d, l], core_peers[i - 1])

    def from_x(d, l):
        for e in range(1, nx):
            block = wg.at[l, back(z, d, nz), back(x, e, nx), c]
            arrived(block, gxr.at[e - 1, d, l])
            for i in range(1, nc):
                send(block, block, gcs.at[i - 1, e, d, l], gcr.at[i - 1, e, d, l], core_peers[i - 1])

    wpeak.relay()
    for d in range(1, nz):
        for l in range(nl):
            from_z(d, l)
        for l in range(nl):
            from_x(d - 1, l)
    for l in range(nl):
        from_x(nz - 1, l)
    peaks = wpeak.finish()
    scales = [1.0 / jnp.full((8, LANES), peaks[l], f32)[:1] for l in range(nl)]

    def norm(zz, xx, cc, l):
        ow_ref[l, zz, xx, cc] = (wg[l, zz, xx, cc].astype(f32) * scales[l]).astype(bf16)

    for l in range(nl):
        for i in range(nz * nx):
            norm(i // nx, i % nx, c, l)
    for d in range(nz):
        for e in range(nx):
            for l in range(nl):
                for i in range(1, nc):
                    block = wg.at[l, back(z, d, nz), back(x, e, nx), back(c, i, nc)]
                    arrived(block, gcr.at[i - 1, e, d, l])
                    norm(back(z, d, nz), back(x, e, nx), back(c, i, nc), l)
    for copy in pending:
        copy.wait_send()


def local(n, nt, grads, moment1, moment2, master):
    nz, nx, nc = split_zero(n)
    nl, rows, width = grads.shape[1:]
    deep = (rows // n) * width // LANES
    dims = (nz, nx, nc, nt, nl)
    g = grads.reshape(nl, n, deep, LANES).reshape(nl, nz, nx, nc, deep, LANES)
    flat = (nl, deep, LANES)
    packed = (deep, nl, LANES)
    peers = nc * nt - 1 + nz * nx - 1
    c1, x1, z1 = max(nc - 1, 1), max(nx - 1, 1), max(nz - 1, 1)
    dma = pltpu.SemaphoreType.DMA
    tile = (nl, 8, LANES)
    vm = pl.BlockSpec(memory_space=pltpu.VMEM)
    sems = [dma((c1, nz, nl))] * 2 + [dma((x1, nz, nl))] * 2 + [dma((z1, nl))] * 2
    sems += [dma((z1, nl))] * 2 + [dma((x1, nz, nl))] * 2 + [dma((c1, nx, nz, nl))] * 2
    sems += [dma((peers,))] * 4
    o1, o2, om, weights = pl.pallas_call(
        functools.partial(kernel, dims),
        out_shape=(
            jax.ShapeDtypeStruct(packed, bf16),
            jax.ShapeDtypeStruct(flat, f32),
            jax.ShapeDtypeStruct(flat, f32),
            jax.ShapeDtypeStruct((nl, nz, nx, nc, deep, LANES), bf16),
        ),
        in_specs=[vm] * 4,
        out_specs=(vm,) * 4,
        scratch_shapes=[
            pltpu.VMEM((nl, nz, nx, nc, deep, LANES), bf16),
            pltpu.VMEM(packed, f32),
            pltpu.VMEM(packed, f32),
            pltpu.VMEM((c1, nz, nl, nx, deep, LANES), bf16),
            pltpu.VMEM((x1, nz) + flat, bf16),
            pltpu.VMEM((x1, nz) + flat, bf16),
            pltpu.VMEM((z1,) + flat, bf16),
            pltpu.VMEM((z1,) + flat, bf16),
            pltpu.VMEM(flat, f32),
            pltpu.VMEM((2,) + tile, f32),
            pltpu.VMEM((peers,) + tile, f32),
            pltpu.VMEM((2,) + tile, f32),
            pltpu.VMEM((peers,) + tile, f32),
        ] + sems,
        compiler_params=pltpu.CompilerParams(collective_id=0, has_side_effects=True, vmem_limit_bytes=16 << 20),
    )(g, moment1.reshape(flat).transpose(1, 0, 2), moment2.reshape(flat), master.reshape(flat))
    shape = moment1.shape
    return (o1.transpose(1, 0, 2).reshape(shape), o2.reshape(shape), om.reshape(shape),
            weights.reshape(nl, rows, width))


def solution(mesh):
    n, nt = mesh.shape["zero"], mesh.shape["tensor"]
    placed = (
        P("zero", None, None, "tensor"),
        P(None, "zero", "tensor"),
        P(None, "zero", "tensor"),
        P(None, "zero", "tensor"),
    )
    return jax.shard_map(
        functools.partial(local, n, nt),
        mesh=mesh,
        in_specs=placed,
        out_specs=(
            P(None, "zero", "tensor"),
            P(None, "zero", "tensor"),
            P(None, "zero", "tensor"),
            P(None, None, "tensor"),
        ),
        check_vma=False,
    )
```

```python
import functools

import jax
import jax.numpy as jnp
from jax import lax
from jax.experimental import pallas as pl
from jax.experimental.pallas import tpu as pltpu
from jax.sharding import PartitionSpec as P

decay_first = 0.9
decay_second = 0.95
learn_rate = 0.001
weight_decay = 0.1
adam_epsilon = 1e-08
peak_epsilon = 1e-06
bias_first = 1.0 - 0.9**10
bias_second = 1.0 - 0.95**10

LANES = 128
CUTS = 2
MESH = pl.DeviceIdType.MESH
f32 = jnp.float32
bf16 = jnp.bfloat16


def split_zero(n):
    nc = 2 if n % 2 == 0 else 1
    m = n // nc
    nx = 1
    while (nx * 2) * (nx * 2) <= m and m % (nx * 2) == 0:
        nx *= 2
    return m // nx, nx, nc


def fold(block):
    return jnp.max(jnp.abs(block.astype(f32)).reshape(-1, 8, LANES), axis=0)


def kernel(dims, g_ref, m1_ref, m2_ref, ms_ref,
           o1_ref, o2_ref, om_ref, ow_ref,
           wg, m1_wide, o1_wide, buf_c, send_x, buf_x, send_z, buf_z, own,
           pk, pk_in, wk, wk_in,
           cs, cr, xs, xr, zs, zr, gzs, gzr, gxs, gxr, gcs, gcr, ps, pr, ws, wr):
    nz, nx, nc, nt, nl, nh = dims
    nk = nl * nh
    me = lax.axis_index("zero")
    te = lax.axis_index("tensor")
    c = lax.rem(me, nc)
    x = lax.rem(lax.div(me, nc), nx)
    z = lax.div(me, nc * nx)

    def at(zz, xx, cc):
        return {"zero": (zz * nx + xx) * nc + cc}

    def turn(v, d, n):
        return lax.rem(v + d, n)

    core_peers = [at(z, x, turn(c, d, nc)) for d in range(1, nc)]
    x_peers = [at(z, turn(x, d, nx), c) for d in range(1, nx)]
    z_peers = [at(turn(z, d, nz), x, c) for d in range(1, nz)]
    t_peers = [{"tensor": turn(te, d, nt)} for d in range(1, nt)]
    near = core_peers + t_peers + [
        {**at(z, x, turn(c, i, nc)), "tensor": turn(te, d, nt)} for i in range(1, nc) for d in range(1, nt)]
    far = [at(turn(z, d, nz), turn(x, e, nx), c) for d in range(nz) for e in range(nx) if d or e]
    pending = []

    def send(src, dst, s, r, to):
        copy = pltpu.make_async_remote_copy(
            src_ref=src, dst_ref=dst, send_sem=s, recv_sem=r,
            device_id=to, device_id_type=MESH)
        copy.start()
        pending.append(copy)

    def arrived(dst, r):
        pltpu.make_async_copy(dst, dst, r).wait()

    barrier = pltpu.get_barrier_semaphore()
    everyone = near + far
    for p in everyone:
        pl.semaphore_signal(barrier, inc=1, device_id=p, device_id_type=MESH)

    class Peak:
        def __init__(self, held, inbox, s, r):
            self.held, self.inbox, self.s, self.r = held, inbox, s, r

        def push(self, stage):
            first = 0 if stage == 0 else len(near)
            for i, p in enumerate(near if stage == 0 else far):
                k = first + i
                send(self.held.at[stage], self.inbox.at[k], self.s.at[k], self.r.at[k], p)

        def pull(self, stage):
            first = 0 if stage == 0 else len(near)
            best = self.held[stage]
            for k in range(first, first + len(near if stage == 0 else far)):
                arrived(self.inbox.at[k], self.r.at[k])
                best = jnp.maximum(best, self.inbox[k])
            return best

        def relay(self):
            self.held[1] = self.pull(0)
            self.push(1)

        def finish(self):
            best = self.pull(1)
            return [jnp.max(best[l]) + peak_epsilon for l in range(nl)]

    for l in range(nl):
        def part(i, best, l=l):
            zz, rest = lax.div(i, nx * nc), lax.rem(i, nx * nc)
            for h in range(nh):
                best = jnp.maximum(best, fold(g_ref[l, zz, lax.div(rest, nc), lax.rem(rest, nc), h]))
            return best
        pk[0, l] = lax.fori_loop(0, nz * nx * nc, part, jnp.zeros((8, LANES), f32))

    pl.semaphore_wait(barrier, len(everyone))

    peak = Peak(pk, pk_in, ps, pr)
    peak.push(0)
    def pair(d, k, xx):
        total = g_ref[k // nh, turn(z, d, nz), xx, c, k % nh].astype(f32)
        for i in range(nc - 1):
            total = total + buf_c[i, d, k, xx].astype(f32)
        return total

    order = list(range(1, nz)) + [0]

    def swap_cores(k):
        for d in order:
            for i in range(1, nc):
                send(g_ref.at[k // nh, turn(z, d, nz), :, turn(c, i, nc), k % nh], buf_c.at[i - 1, d, k],
                     cs.at[i - 1, d, k], cr.at[i - 1, d, k], core_peers[i - 1])

    def reduce_core(k):
        for d in order:
            for i in range(nc - 1):
                arrived(buf_c.at[i, d, k], cr.at[i, d, k])
            for e in range(1, nx):
                send_x[e - 1, d, k] = pair(d, k, turn(x, e, nx)).astype(bf16)
                send(send_x.at[e - 1, d, k], buf_x.at[e - 1, d, k],
                     xs.at[e - 1, d, k], xr.at[e - 1, d, k], x_peers[e - 1])

    def reduce_x(k):
        for d in order:
            for e in range(1, nx):
                arrived(buf_x.at[e - 1, d, k], xr.at[e - 1, d, k])
            total = pair(d, k, x)
            for e in range(1, nx):
                total = total + buf_x[e - 1, d, k].astype(f32)
            if d:
                send_z[d - 1, k] = total.astype(bf16)
                send(send_z.at[d - 1, k], buf_z.at[d - 1, k], zs.at[d - 1, k], zr.at[d - 1, k], z_peers[d - 1])
            else:
                own[k] = total

    up, down = z < nz - 1, z > 0
    ways = [(up, 1), (down, -1)]

    def came(s, way):
        return z >= s if way == 0 else z + s < nz

    def onward(block, s, way, k):
        go, sign = ways[way]

        @pl.when(go)
        def _():
            hop = pltpu.make_async_remote_copy(
                src_ref=block, dst_ref=block, send_sem=gzs.at[way, s, k], recv_sem=gzr.at[way, s, k],
                device_id=at(z + sign, x, c), device_id_type=MESH)
            hop.start()

    def spread(block, slot, k):
        for e in range(1, nx):
            pltpu.make_async_remote_copy(
                src_ref=block, dst_ref=block, send_sem=gxs.at[e - 1, slot, k], recv_sem=gxr.at[e - 1, slot, k],
                device_id=x_peers[e - 1], device_id_type=MESH).start()
        for i in range(1, nc):
            pltpu.make_async_remote_copy(
                src_ref=block, dst_ref=block, send_sem=gcs.at[i - 1, 0, slot, k],
                recv_sem=gcr.at[i - 1, 0, slot, k],
                device_id=core_peers[i - 1], device_id_type=MESH).start()

    def view(k, zz, xx, cc):
        return wg.at[k // nh, zz, xx, cc, k % nh]

    def source(slot):
        if slot == 0:
            return z
        s, way = (slot + 1) // 2, (slot - 1) % 2
        return z - s if way == 0 else z + s

    def update(k):
        l, h = k // nh, k % nh
        total = own[k]
        for d in range(1, nz):
            arrived(buf_z.at[d - 1, k], zr.at[d - 1, k])
            total = total + buf_z[d - 1, k].astype(f32)
        gsum = total / peaks[l]
        first = (decay_first * m1_wide[h, :, l, :] + (1.0 - decay_first) * gsum).astype(bf16)
        second = decay_second * m2_ref[k] + (1.0 - decay_second) * gsum * gsum
        step_dir = first.astype(f32) / bias_first / (jnp.sqrt(second / bias_second) + adam_epsilon)
        master = ms_ref[k]
        fresh = master - learn_rate * (step_dir + weight_decay * master)
        wg[l, z, x, c, h] = fresh.astype(bf16)
        mine = view(k, z, x, c)
        onward(mine, 0, 0, k)
        onward(mine, 0, 1, k)
        spread(mine, 0, k)
        om_ref[k] = fresh
        o2_ref[k] = second
        o1_wide[h, :, l, :] = first.astype(f32)
        best = fold(fresh)
        wk[0, l] = best if h == 0 else jnp.maximum(wk[0, l], best)

    def gather_z(k, s):
        for way in (0, 1):
            @pl.when(came(s, way))
            def _(way=way):
                slot = 2 * s - 1 + way
                block = view(k, source(slot), x, c)
                arrived(block, gzr.at[way, s - 1, k])
                if s < nz - 1:
                    onward(block, s, way, k)
                spread(block, slot, k)

    def each_slot(s, act):
        if s == 0:
            act(0)
            return
        for way in (0, 1):
            @pl.when(came(s, way))
            def _(way=way):
                act(2 * s - 1 + way)

    def gather_x(k, s):
        def act(slot):
            for e in range(1, nx):
                block = view(k, source(slot), lax.rem(x + nx - e, nx), c)
                arrived(block, gxr.at[e - 1, slot, k])
                for i in range(1, nc):
                    pltpu.make_async_remote_copy(
                        src_ref=block, dst_ref=block, send_sem=gcs.at[i - 1, e, slot, k],
                        recv_sem=gcr.at[i - 1, e, slot, k],
                        device_id=core_peers[i - 1], device_id_type=MESH).start()
        each_slot(s, act)

    for k in range(nk):
        swap_cores(k)
    m1_wide[...] = m1_ref[...].astype(f32)
    reduce_core(0)
    peak.relay()
    for k in range(1, nk):
        reduce_core(k)
    wpeak = Peak(wk, wk_in, ws, wr)
    peaks = []

    def stage(number, k):
        if not 0 <= k < nk:
            return
        if number == 0:
            reduce_x(k)
        elif number == 1:
            if k == 0:
                peaks.extend(peak.finish())
            update(k)
            if k == nk - 1:
                wpeak.push(0)
        elif number == 2:
            gather_z(k, 1)
            gather_x(k, 0)
        else:
            if number == 3 and k == nk - 1:
                wpeak.relay()
            s = number - 1
            if s < nz:
                gather_z(k, s)
            gather_x(k, s - 1)

    last = nz + 1
    for t in range(nk + last + 1):
        for number in range(last, -1, -1):
            stage(number, t - number)
    o1_ref[...] = o1_wide[...].astype(bf16)
    top = wpeak.finish()
    scales = [1.0 / jnp.full((8, LANES), top[l], f32)[:1] for l in range(nl)]

    def norm(l, zz, xx, cc, h):
        ow_ref[l, zz, xx, cc, h] = (wg[l, zz, xx, cc, h].astype(f32) * scales[l]).astype(bf16)

    for k in range(nk):
        for i in range(nz * nx):
            norm(k // nh, i // nx, i % nx, c, k % nh)
    for k in range(nk):
        for s in range(nz):
            def act(slot, k=k):
                for e in range(nx):
                    xx = lax.rem(x + nx - e, nx)
                    for i in range(1, nc):
                        cc = lax.rem(c + nc - i, nc)
                        arrived(view(k, source(slot), xx, cc), gcr.at[i - 1, e, slot, k])
                        norm(k // nh, source(slot), xx, cc, k % nh)
            each_slot(s, act)

    one = view(0, z, x, c)

    def left(sem):
        pltpu.make_async_copy(one, one, sem).wait()

    for k in range(nk):
        for way in (0, 1):
            @pl.when(ways[way][0])
            def _(k=k, way=way):
                left(gzs.at[way, 0, k])
                for s in range(1, nz - 1):
                    @pl.when(came(s, way))
                    def _(s=s):
                        left(gzs.at[way, s, k])
        for s in range(nz):
            def gone(slot, k=k):
                for e in range(1, nx):
                    left(gxs.at[e - 1, slot, k])
                for i in range(1, nc):
                    for e in range(nx):
                        left(gcs.at[i - 1, e, slot, k])
            each_slot(s, gone)
    for copy in pending:
        copy.wait_send()


def local(n, nt, grads, moment1, moment2, master):
    nz, nx, nc = split_zero(n)
    nl, rows, width = grads.shape[1:]
    deep = (rows // n) * width // LANES
    nh = next((h for h in (CUTS, 3, 2) if deep % (16 * h) == 0), 1)
    nk, dh = nl * nh, deep // nh
    dims = (nz, nx, nc, nt, nl, nh)
    whole = (nl, nz, nx, nc, nh, dh, LANES)
    flat = (nk, dh, LANES)
    packed = (nh, dh, nl, LANES)
    peers = nc * nt - 1 + nz * nx - 1
    c1, x1, z1 = max(nc - 1, 1), max(nx - 1, 1), max(nz - 1, 1)
    slots = 2 * nz - 1
    dma = pltpu.SemaphoreType.DMA
    tile = (nl, 8, LANES)
    vm = pl.BlockSpec(memory_space=pltpu.VMEM)
    sems = [dma((c1, nz, nk))] * 2 + [dma((x1, nz, nk))] * 2 + [dma((z1, nk))] * 2
    sems += [dma((2, z1, nk))] * 2 + [dma((x1, slots, nk))] * 2 + [dma((c1, nx, slots, nk))] * 2
    sems += [dma((peers,))] * 4
    o1, o2, om, weights = pl.pallas_call(
        functools.partial(kernel, dims),
        out_shape=(
            jax.ShapeDtypeStruct(packed, bf16),
            jax.ShapeDtypeStruct(flat, f32),
            jax.ShapeDtypeStruct(flat, f32),
            jax.ShapeDtypeStruct(whole, bf16),
        ),
        in_specs=[vm] * 4,
        out_specs=(vm,) * 4,
        scratch_shapes=[
            pltpu.VMEM(whole, bf16),
            pltpu.VMEM(packed, f32),
            pltpu.VMEM(packed, f32),
            pltpu.VMEM((c1, nz, nk, nx, dh, LANES), bf16),
            pltpu.VMEM((x1, nz) + flat, bf16),
            pltpu.VMEM((x1, nz) + flat, bf16),
            pltpu.VMEM((z1,) + flat, bf16),
            pltpu.VMEM((z1,) + flat, bf16),
            pltpu.VMEM(flat, f32),
            pltpu.VMEM((2,) + tile, f32),
            pltpu.VMEM((peers,) + tile, f32),
            pltpu.VMEM((2,) + tile, f32),
            pltpu.VMEM((peers,) + tile, f32),
        ] + sems,
        compiler_params=pltpu.CompilerParams(collective_id=0, has_side_effects=True, vmem_limit_bytes=16 << 20),
    )(grads.reshape(whole), moment1.reshape(nl, nh, dh, LANES).transpose(1, 2, 0, 3),
      moment2.reshape(flat), master.reshape(flat))
    shape = moment1.shape
    return (o1.transpose(2, 0, 1, 3).reshape(shape), o2.reshape(shape), om.reshape(shape),
            weights.reshape(nl, rows, width))


def solution(mesh):
    n, nt = mesh.shape["zero"], mesh.shape["tensor"]
    placed = (
        P("zero", None, None, "tensor"),
        P(None, "zero", "tensor"),
        P(None, "zero", "tensor"),
        P(None, "zero", "tensor"),
    )
    return jax.shard_map(
        functools.partial(local, n, nt),
        mesh=mesh,
        in_specs=placed,
        out_specs=(
            P(None, "zero", "tensor"),
            P(None, "zero", "tensor"),
            P(None, "zero", "tensor"),
            P(None, None, "tensor"),
        ),
        check_vma=False,
    )
```

```python
import functools

import jax
import jax.numpy as jnp
from jax import lax
from jax.experimental import pallas as pl
from jax.experimental.pallas import tpu as pltpu
from jax.sharding import PartitionSpec as P

decay_first = 0.9
decay_second = 0.95
learn_rate = 0.001
weight_decay = 0.1
adam_epsilon = 1e-08
peak_epsilon = 1e-06
bias_first = 1.0 - 0.9**10
bias_second = 1.0 - 0.95**10

LANES = 128
CUTS = 1
STEP, LAG, HOP = 8.4, 20, 20
MESH = pl.DeviceIdType.MESH
f32 = jnp.float32
bf16 = jnp.bfloat16


def split_zero(n):
    nc = 2 if n % 2 == 0 else 1
    m = n // nc
    nx = 1
    while (nx * 2) * (nx * 2) <= m and m % (nx * 2) == 0:
        nx *= 2
    return m // nx, nx, nc


def fold(block):
    return jnp.max(jnp.abs(block.astype(f32)).reshape(-1, 8, LANES), axis=0)


def kernel(dims, g_ref, m1_ref, m2_ref, ms_ref,
           o1_ref, o2_ref, om_ref, ow_ref,
           wg, m1_wide, o1_wide, buf_c, send_x, buf_x, send_z, buf_z, own,
           pk, pk_in, wk, wk_in,
           cs, cr, xs, xr, zs, zr, gzs, gzr, gxs, gxr, gcs, gcr, ps, pr, ws, wr):
    nz, nx, nc, nt, nl, nh = dims
    nk = nl * nh
    me = lax.axis_index("zero")
    te = lax.axis_index("tensor")
    c = lax.rem(me, nc)
    x = lax.rem(lax.div(me, nc), nx)
    z = lax.div(me, nc * nx)

    def at(zz, xx, cc):
        return {"zero": (zz * nx + xx) * nc + cc}

    def turn(v, d, n):
        return lax.rem(v + d, n)

    core_peers = [at(z, x, turn(c, d, nc)) for d in range(1, nc)]
    x_peers = [at(z, turn(x, d, nx), c) for d in range(1, nx)]
    z_peers = [at(turn(z, d, nz), x, c) for d in range(1, nz)]
    t_peers = [{"tensor": turn(te, d, nt)} for d in range(1, nt)]
    near = core_peers + t_peers + [
        {**at(z, x, turn(c, i, nc)), "tensor": turn(te, d, nt)} for i in range(1, nc) for d in range(1, nt)]
    far = [at(turn(z, d, nz), turn(x, e, nx), c) for d in range(nz) for e in range(nx) if d or e]
    pending = []

    def send(src, dst, s, r, to):
        copy = pltpu.make_async_remote_copy(
            src_ref=src, dst_ref=dst, send_sem=s, recv_sem=r,
            device_id=to, device_id_type=MESH)
        copy.start()
        pending.append(copy)

    def arrived(dst, r):
        pltpu.make_async_copy(dst, dst, r).wait()

    barrier = pltpu.get_barrier_semaphore()
    everyone = near + far
    for p in everyone:
        pl.semaphore_signal(barrier, inc=1, device_id=p, device_id_type=MESH)

    class Peak:
        def __init__(self, held, inbox, s, r):
            self.held, self.inbox, self.s, self.r = held, inbox, s, r

        def push(self, stage):
            first = 0 if stage == 0 else len(near)
            for i, p in enumerate(near if stage == 0 else far):
                k = first + i
                send(self.held.at[stage], self.inbox.at[k], self.s.at[k], self.r.at[k], p)

        def pull(self, stage):
            first = 0 if stage == 0 else len(near)
            best = self.held[stage]
            for k in range(first, first + len(near if stage == 0 else far)):
                arrived(self.inbox.at[k], self.r.at[k])
                best = jnp.maximum(best, self.inbox[k])
            return best

        def relay(self):
            self.held[1] = self.pull(0)
            self.push(1)

        def finish(self):
            best = self.pull(1)
            return [jnp.max(best[l]) + peak_epsilon for l in range(nl)]

    for l in range(nl):
        def part(i, best, l=l):
            zz, rest = lax.div(i, nx * nc), lax.rem(i, nx * nc)
            for h in range(nh):
                best = jnp.maximum(best, fold(g_ref[l, zz, lax.div(rest, nc), lax.rem(rest, nc), h]))
            return best
        pk[0, l] = lax.fori_loop(0, nz * nx * nc, part, jnp.zeros((8, LANES), f32))

    pl.semaphore_wait(barrier, len(everyone))

    peak = Peak(pk, pk_in, ps, pr)
    peak.push(0)
    def pair(d, k, xx):
        total = g_ref[k // nh, turn(z, d, nz), xx, c, k % nh].astype(f32)
        for i in range(nc - 1):
            total = total + buf_c[i, d, k, xx].astype(f32)
        return total

    order = list(range(1, nz)) + [0]

    def swap_cores(k):
        for d in order:
            for i in range(1, nc):
                send(g_ref.at[k // nh, turn(z, d, nz), :, turn(c, i, nc), k % nh], buf_c.at[i - 1, d, k],
                     cs.at[i - 1, d, k], cr.at[i - 1, d, k], core_peers[i - 1])

    def reduce_core(k):
        for d in order:
            for i in range(nc - 1):
                arrived(buf_c.at[i, d, k], cr.at[i, d, k])
            for e in range(1, nx):
                send_x[e - 1, d, k] = pair(d, k, turn(x, e, nx)).astype(bf16)
                send(send_x.at[e - 1, d, k], buf_x.at[e - 1, d, k],
                     xs.at[e - 1, d, k], xr.at[e - 1, d, k], x_peers[e - 1])

    def reduce_x(k):
        for d in order:
            for e in range(1, nx):
                arrived(buf_x.at[e - 1, d, k], xr.at[e - 1, d, k])
            total = pair(d, k, x)
            for e in range(1, nx):
                total = total + buf_x[e - 1, d, k].astype(f32)
            if d:
                send_z[d - 1, k] = total.astype(bf16)
                send(send_z.at[d - 1, k], buf_z.at[d - 1, k], zs.at[d - 1, k], zr.at[d - 1, k], z_peers[d - 1])
            else:
                own[k] = total

    up, down = z < nz - 1, z > 0
    ways = [(up, 1), (down, -1)]

    def came(s, way):
        return z >= s if way == 0 else z + s < nz

    def onward(block, s, way, k):
        go, sign = ways[way]

        @pl.when(go)
        def _():
            hop = pltpu.make_async_remote_copy(
                src_ref=block, dst_ref=block, send_sem=gzs.at[way, s, k], recv_sem=gzr.at[way, s, k],
                device_id=at(z + sign, x, c), device_id_type=MESH)
            hop.start()

    def spread(block, slot, k):
        for e in range(1, nx):
            pltpu.make_async_remote_copy(
                src_ref=block, dst_ref=block, send_sem=gxs.at[e - 1, slot, k], recv_sem=gxr.at[e - 1, slot, k],
                device_id=x_peers[e - 1], device_id_type=MESH).start()

    def line(k, zz, cc):
        return wg.at[k // nh, zz, :, cc, k % nh]

    def view(k, zz, xx, cc):
        return wg.at[k // nh, zz, xx, cc, k % nh]

    def source(slot):
        if slot == 0:
            return z
        s, way = (slot + 1) // 2, (slot - 1) % 2
        return z - s if way == 0 else z + s

    def update(k):
        l, h = k // nh, k % nh
        total = own[k]
        for d in range(1, nz):
            arrived(buf_z.at[d - 1, k], zr.at[d - 1, k])
            total = total + buf_z[d - 1, k].astype(f32)
        gsum = total / peaks[l]
        first = (decay_first * m1_wide[h, :, l, :] + (1.0 - decay_first) * gsum).astype(bf16)
        second = decay_second * m2_ref[k] + (1.0 - decay_second) * gsum * gsum
        step_dir = first.astype(f32) / bias_first / (jnp.sqrt(second / bias_second) + adam_epsilon)
        master = ms_ref[k]
        fresh = master - learn_rate * (step_dir + weight_decay * master)
        wg[l, z, x, c, h] = fresh.astype(bf16)
        mine = view(k, z, x, c)
        onward(mine, 0, 0, k)
        onward(mine, 0, 1, k)
        spread(mine, 0, k)
        om_ref[k] = fresh
        o2_ref[k] = second
        o1_wide[h, :, l, :] = first.astype(f32)
        best = fold(fresh)
        wk[0, l] = best if h == 0 else jnp.maximum(wk[0, l], best)

    def gather_z(k, s):
        for way in (0, 1):
            @pl.when(came(s, way))
            def _(way=way):
                slot = 2 * s - 1 + way
                block = view(k, source(slot), x, c)
                arrived(block, gzr.at[way, s - 1, k])
                if s < nz - 1:
                    onward(block, s, way, k)
                spread(block, slot, k)

    def each_slot(s, act):
        if s == 0:
            act(0)
            return
        for way in (0, 1):
            @pl.when(came(s, way))
            def _(way=way):
                act(2 * s - 1 + way)

    def gather_x(k, s):
        def act(slot):
            for e in range(1, nx):
                block = view(k, source(slot), lax.rem(x + nx - e, nx), c)
                arrived(block, gxr.at[e - 1, slot, k])
            blocks = line(k, source(slot), c)
            for i in range(1, nc):
                pltpu.make_async_remote_copy(
                    src_ref=blocks, dst_ref=blocks, send_sem=gcs.at[i - 1, slot, k],
                    recv_sem=gcr.at[i - 1, slot, k],
                    device_id=core_peers[i - 1], device_id_type=MESH).start()
        each_slot(s, act)

    for k in range(nk):
        swap_cores(k)
    m1_wide[...] = m1_ref[...].astype(f32)
    reduce_core(0)
    peak.relay()
    for k in range(1, nk):
        reduce_core(k)
    wpeak = Peak(wk, wk_in, ws, wr)
    peaks = []

    def stage(number, k):
        if not 0 <= k < nk:
            return
        if number == 0:
            reduce_x(k)
        elif number == 1:
            if k == 0:
                peaks.extend(peak.finish())
            update(k)
            if k == nk - 1:
                wpeak.push(0)
        elif number == 2:
            gather_z(k, 1)
            gather_x(k, 0)
        else:
            if number == 3 and k == nk - 1:
                wpeak.relay()
            s = number - 1
            if s < nz:
                gather_z(k, s)
            gather_x(k, s - 1)

    due = []
    for k in range(nk):
        begun = STEP * k / nk
        for number in range(nz + 2):
            due.append((begun + (LAG + HOP * (number - 1) if number else 0), k, number))
    for _, k, number in sorted(due):
        stage(number, k)
    o1_ref[...] = o1_wide[...].astype(bf16)
    top = wpeak.finish()
    scales = [1.0 / jnp.full((8, LANES), top[l], f32)[:1] for l in range(nl)]

    def norm(l, zz, xx, cc, h):
        ow_ref[l, zz, xx, cc, h] = (wg[l, zz, xx, cc, h].astype(f32) * scales[l]).astype(bf16)

    for k in range(nk):
        for i in range(nz * nx):
            norm(k // nh, i // nx, i % nx, c, k % nh)
    for k in range(nk):
        for s in range(nz):
            def act(slot, k=k):
                for i in range(1, nc):
                    cc = lax.rem(c + nc - i, nc)
                    arrived(line(k, source(slot), cc), gcr.at[i - 1, slot, k])
                    for xx in range(nx):
                        norm(k // nh, source(slot), xx, cc, k % nh)
            each_slot(s, act)

    one = view(0, z, x, c)

    def left(sem):
        pltpu.make_async_copy(one, one, sem).wait()

    for k in range(nk):
        for way in (0, 1):
            @pl.when(ways[way][0])
            def _(k=k, way=way):
                left(gzs.at[way, 0, k])
                for s in range(1, nz - 1):
                    @pl.when(came(s, way))
                    def _(s=s):
                        left(gzs.at[way, s, k])
        for s in range(nz):
            def gone(slot, k=k):
                for e in range(1, nx):
                    left(gxs.at[e - 1, slot, k])
                for i in range(1, nc):
                    lot = line(0, z, c)
                    pltpu.make_async_copy(lot, lot, gcs.at[i - 1, slot, k]).wait()
            each_slot(s, gone)
    for copy in pending:
        copy.wait_send()


def hand_on(a_ref, b_ref, c_ref, x_ref, y_ref, z_ref):
    x_ref[...] = a_ref[...]
    y_ref[...] = b_ref[...]
    z_ref[...] = c_ref[...]


def local(n, nt, grads, moment1, moment2, master):
    nz, nx, nc = split_zero(n)
    nl, rows, width = grads.shape[1:]
    deep = (rows // n) * width // LANES
    nh = next((h for h in (CUTS, 3, 2) if deep % (16 * h) == 0), 1)
    nk, dh = nl * nh, deep // nh
    dims = (nz, nx, nc, nt, nl, nh)
    whole = (nl, nz, nx, nc, nh, dh, LANES)
    flat = (nk, dh, LANES)
    packed = (nh, dh, nl, LANES)
    peers = nc * nt - 1 + nz * nx - 1
    c1, x1, z1 = max(nc - 1, 1), max(nx - 1, 1), max(nz - 1, 1)
    slots = 2 * nz - 1
    dma = pltpu.SemaphoreType.DMA
    tile = (nl, 8, LANES)
    vm = pl.BlockSpec(memory_space=pltpu.VMEM)
    sems = [dma((c1, nz, nk))] * 2 + [dma((x1, nz, nk))] * 2 + [dma((z1, nk))] * 2
    sems += [dma((2, z1, nk))] * 2 + [dma((x1, slots, nk))] * 2 + [dma((c1, slots, nk))] * 2
    sems += [dma((peers,))] * 4
    o1, o2, om, weights = pl.pallas_call(
        functools.partial(kernel, dims),
        out_shape=(
            jax.ShapeDtypeStruct(packed, bf16),
            jax.ShapeDtypeStruct(flat, f32),
            jax.ShapeDtypeStruct(flat, f32),
            jax.ShapeDtypeStruct(whole, bf16),
        ),
        in_specs=[vm] * 4,
        out_specs=(vm,) * 4,
        scratch_shapes=[
            pltpu.VMEM(whole, bf16),
            pltpu.VMEM(packed, f32),
            pltpu.VMEM(packed, f32),
            pltpu.VMEM((c1, nz, nk, nx, dh, LANES), bf16),
            pltpu.VMEM((x1, nz) + flat, bf16),
            pltpu.VMEM((x1, nz) + flat, bf16),
            pltpu.VMEM((z1,) + flat, bf16),
            pltpu.VMEM((z1,) + flat, bf16),
            pltpu.VMEM(flat, f32),
            pltpu.VMEM((2,) + tile, f32),
            pltpu.VMEM((peers,) + tile, f32),
            pltpu.VMEM((2,) + tile, f32),
            pltpu.VMEM((peers,) + tile, f32),
        ] + sems,
        compiler_params=pltpu.CompilerParams(collective_id=0, has_side_effects=True, vmem_limit_bytes=16 << 20),
    )(grads.reshape(whole), moment1.reshape(nl, nh, dh, LANES).transpose(1, 2, 0, 3),
      moment2.reshape(flat), master.reshape(flat))
    o1, o2, om = pl.pallas_call(
        hand_on,
        out_shape=tuple(jax.ShapeDtypeStruct(v.shape, v.dtype) for v in (o1, o2, om)),
        in_specs=[vm] * 3,
        out_specs=(vm,) * 3,
        compiler_params=pltpu.CompilerParams(vmem_limit_bytes=4 << 20),
    )(o1, o2, om)
    shape = moment1.shape
    return (o1.transpose(2, 0, 1, 3).reshape(shape), o2.reshape(shape), om.reshape(shape),
            weights.reshape(nl, rows, width))


def solution(mesh):
    n, nt = mesh.shape["zero"], mesh.shape["tensor"]
    placed = (
        P("zero", None, None, "tensor"),
        P(None, "zero", "tensor"),
        P(None, "zero", "tensor"),
        P(None, "zero", "tensor"),
    )
    return jax.shard_map(
        functools.partial(local, n, nt),
        mesh=mesh,
        in_specs=placed,
        out_specs=(
            P(None, "zero", "tensor"),
            P(None, "zero", "tensor"),
            P(None, "zero", "tensor"),
            P(None, None, "tensor"),
        ),
        check_vma=False,
    )
```
